32 devices in a mesh: replica: 8 (over z, y), expert: 4 (over x, core).
Axes of the slice: x: 2, y: 2, z: 4, core: 2. Of those that a mesh axis runs over, the one named last changes fastest.
Arguments:
- outer_params: float32 [28672, 4096], P('expert', 'replica'), may hold values from -6 to 6
- momentum: bfloat16 [28672, 4096], P('expert', 'replica'), may hold values from -6 to 6
- replica_deltas: bfloat16 [8, 8, 128, 4096], P('replica', 'expert'), may hold values from -6 to 6
- replica_rows: bfloat16 [8, 8, 128, 4096], P('replica', 'expert'), may hold values from -6 to 6
- block_ids: int32 [8, 8], P('replica', 'expert'), may hold values from 0 to 223, as said below
- slot_counts: int32 [8, 4], P('replica', 'expert'), may hold values from 0 to 2, as said below
Outputs:
- new_params: float32 [28672, 4096], P('expert', 'replica')
- new_momentum: bfloat16 [28672, 4096], P('expert', 'replica')
- blended_rows: bfloat16 [8, 8, 128, 4096], P('replica', 'expert')
The draws below stay inside these ranges and needn't reach their ends.
Inputs may be any that keep to these rules, and one draw needn't show every extreme that they name: `block_ids`: within row r, slots e * 2 to (e + 1) * 2 - 1 name distinct blocks among e * 56 to (e + 1) * 56 - 1. The first slot_counts[r, e] slots of group e of row r are live, the rest are padding; in every draw some index e has 2 in every row.
All inputs are finite; a program needn't handle non-finite values.
Results may differ from the reference program's by a relative error of at most 0.0075.
Values may be sent and summed in bfloat16 or wider, within the bound.
No kernel may reach another device: no remote copies, remote signals or barrier semaphores. Data moves between devices by JAX's collectives and lax.ppermute only.
A program may use at most 128 MiB of HBM per device.

```python
import jax
import jax.numpy as jnp
from jax import lax

D = 4096
BLOCK = 128
MAXB = 2
REPLICAS = 8
ROWS = 28672
LB = 56
SLOTS = 8
N_EXPERT = 4


def draw_block_ids(key, part):
    scores = jax.random.randint(jax.random.fold_in(key, 11), (REPLICAS, N_EXPERT, LB), 0, 1048576)
    scores = scores * LB + jnp.arange(LB, dtype=jnp.int32)[None, None, :]
    order = jnp.argsort(scores, axis=2, stable=True)[:, :, :MAXB].astype(jnp.int32)
    offsets = (jnp.arange(N_EXPERT, dtype=jnp.int32) * LB)[None, :, None]
    return (order + offsets).reshape(REPLICAS, N_EXPERT * MAXB)


def draw_slot_counts(key, part):
    counts = jax.random.randint(jax.random.fold_in(key, 23), (REPLICAS, N_EXPERT), 0, MAXB + 1)
    hottest = jax.random.randint(jax.random.fold_in(key, 37), (), 0, N_EXPERT)
    column = jnp.arange(N_EXPERT, dtype=jnp.int32)[None, :]
    return jnp.where(column == hottest, MAXB, counts).astype(jnp.int32)


def steps_of(key, shape, pieces, smallest, top_value):
    factor_of = 1.0
    for position, blocks in pieces:
        draws = jax.random.uniform(jax.random.fold_in(jax.random.fold_in(key, 6), position), (blocks,), jnp.float32, smallest / len(pieces), top_value / len(pieces))
        factor_of = factor_of * jnp.repeat(jnp.exp(draws), shape[position] // blocks).reshape((-1,) + (1,) * (len(shape) - 1 - position))
    return factor_of


def noise(rng, shape, spread, limit, split=(), kind=jnp.bfloat16):
    factor_of = steps_of(rng, shape, split, -0.22, 0.18) if split else 1.0
    drawn = jax.random.normal(rng, shape, jnp.float32) * spread * factor_of
    return jnp.minimum(jnp.maximum(drawn, -limit), limit).astype(kind)


def setup_inputs(seed: int = 0) -> dict:
    key_list = jax.random.split(jax.random.key(seed), 7)
    outer_params = noise(key_list[0], (ROWS, D), 1.0, 6.0, ((0, 4), (1, 8)), jnp.float32)
    momentum = noise(key_list[1], (ROWS, D), 1.0, 6.0, ((0, 4), (1, 8)))
    replica_deltas = noise(key_list[2], (REPLICAS, SLOTS, BLOCK, D), 1.0, 6.0, ((0, 8), (1, 4)))
    replica_rows = noise(key_list[3], (REPLICAS, SLOTS, BLOCK, D), 1.0, 6.0, ((0, 8), (1, 4)))
    block_ids = draw_block_ids(jax.random.fold_in(key_list[6], 71), 0)
    slot_counts = draw_slot_counts(jax.random.fold_in(key_list[6], 71), 0)
    return {"outer_params": outer_params, "momentum": momentum, "replica_deltas": replica_deltas, "replica_rows": replica_rows, "block_ids": block_ids, "slot_counts": slot_counts}


outer_rate = 0.7
nesterov_decay = 0.9
blend_weight = 0.5


def reference(outer_params, momentum, replica_deltas, replica_rows, block_ids, slot_counts):
    block_total = ROWS // BLOCK
    slot_index = jnp.arange(SLOTS, dtype=jnp.int32) % MAXB
    group_index = jnp.arange(SLOTS, dtype=jnp.int32) // MAXB
    active = slot_index[None, :] < slot_counts[:, group_index]

    def accumulate(carry, inputs):
        totals, tallies = carry
        deltas, listed, flags = inputs
        weights = flags.astype(jnp.float32)
        totals = totals.at[listed].add(deltas.astype(jnp.float32) * weights[:, None, None])
        tallies = tallies.at[listed].add(weights)
        return (totals, tallies), None

    start = (jnp.zeros((block_total, BLOCK, D), jnp.float32), jnp.zeros((block_total,), jnp.float32))
    (totals, tallies), unused = lax.scan(accumulate, start, (replica_deltas, block_ids, active))
    mean_delta = (totals / jnp.maximum(tallies, 1.0)[:, None, None]).reshape(ROWS, D)
    moment = nesterov_decay * momentum.astype(jnp.float32) + mean_delta
    params_new = outer_params - outer_rate * (mean_delta + nesterov_decay * moment)
    blocks_new = params_new.reshape(block_total, BLOCK, D)

    def blend_one(inputs):
        rows, listed, flags = inputs
        fetched = lax.optimization_barrier(blocks_new[listed].astype(jnp.bfloat16)).astype(jnp.float32)
        rows_float = rows.astype(jnp.float32)
        mixed = blend_weight * rows_float + (1.0 - blend_weight) * fetched
        return jnp.where(flags[:, None, None], mixed, rows_float).astype(jnp.bfloat16)

    blended = lax.map(blend_one, (replica_rows, block_ids, active))
    return params_new, moment.astype(jnp.bfloat16), blended
```

```python
import functools

import jax
import jax.numpy as jnp
from jax import lax
from jax.experimental import pallas as pl
from jax.experimental.pallas import tpu as pltpu
from jax.sharding import PartitionSpec as P

outer_rate = 0.7
nesterov_decay = 0.9
blend_weight = 0.5


HBM = pl.BlockSpec(memory_space=pltpu.HBM)
ANY = pl.BlockSpec(memory_space=pl.ANY)
SMEM = pl.BlockSpec(memory_space=pltpu.SMEM)
VMEM = pl.BlockSpec(memory_space=pltpu.VMEM)
DMA = pltpu.SemaphoreType.DMA
BLOCK_BYTES = 1 << 20
PARTS = 2


def peer_of(me, k, n):
    return me ^ k if n & (n - 1) == 0 else (k - me) % n


def rounds_of(n):
    return sorted(range(n), key=lambda k: (k < n // 2, -(k < n // 2) * (n - k), k))


def peer_in_kernel(k, n):
    me = lax.axis_index("replica")
    return me ^ k if n & (n - 1) == 0 else lax.rem(k - me + n, n)


def step_of(mean, momentum, params):
    moment = nesterov_decay * momentum.astype(jnp.float32) + mean
    return moment, params - outer_rate * (mean + nesterov_decay * moment)


def columns_of(k, n, width):
    return pl.ds(pl.multiple_of(peer_in_kernel(k, n) * width, width), width)


def pack_kernel(start, deltas, *rest):
    packed, sems = rest[:-1], rest[-1]
    n, (_, rows, width) = len(packed), packed[0].shape
    copies = [
        pltpu.make_async_copy(
            deltas.at[:, pl.ds(start, rows), columns_of(k, n, width)], packed[k], sems.at[k]
        )
        for k in range(n)
    ]
    for copy in copies:
        copy.start()
    for copy in copies:
        copy.wait()


def pack(deltas, start, rows, n):
    slots, _, total = deltas.shape
    return pl.pallas_call(
        functools.partial(pack_kernel, start),
        name="pack",
        in_specs=[HBM],
        out_specs=[VMEM] * n,
        out_shape=[jax.ShapeDtypeStruct((slots, rows, total // n), deltas.dtype)] * n,
        scratch_shapes=[DMA((n,))],
    )(deltas)


def listed_body(start, block_size, block_count, n, *refs):
    facts, params, momentum = refs[:3]
    received, fetched, means = refs[3 : 3 + n], refs[3 + n : 3 + 2 * n], refs[3 + 2 * n]
    ids, keys, got, held, moved, total, sent, got_sems, held_sems, moved_sems, mean_sems, sent_sems = refs[4 + 2 * n :]
    entries, rows, width = held.shape
    slots = entries // n
    base = lax.axis_index("expert") * block_count

    def place(s):
        return pl.ds(pl.multiple_of(ids[s] * block_size + start, 16), rows)

    def pair(s):
        return (
            pltpu.make_async_copy(params.at[place(s), :], held.at[s], held_sems.at[s]),
            pltpu.make_async_copy(momentum.at[place(s), :], moved.at[s], moved_sems.at[s]),
        )

    arrivals = [
        pltpu.make_async_copy(received[k], got.at[pl.ds(k * slots, slots)], got_sems.at[k]) for k in range(n)
    ]
    for k in range(n):
        arrivals[k].start()
        replica = peer_in_kernel(k, n)
        for j in range(slots):
            s = k * slots + j
            mine = facts[replica, j] - base
            ids[s] = mine
            keys[s] = jnp.where(facts[replica, slots] > j, mine, -1)
            for copy in pair(s):
                copy.start()
    for copy in arrivals:
        copy.wait()

    def work(s, carry):
        mine = ids[s]
        live = (keys[s] == mine).astype(jnp.int32)
        total[s] = got[s].astype(jnp.float32) * live.astype(jnp.float32)

        def add(other, tally):
            match = jnp.logical_and(keys[other] == mine, other != s)

            @pl.when(match)
            def _():
                total[s] += got[other].astype(jnp.float32)

            return tally + match.astype(jnp.int32)

        tally = lax.fori_loop(0, entries, add, live, unroll=8)
        scale = 1.0 / jnp.full((1, width), jnp.maximum(tally, 1).astype(jnp.float32))
        mean = total[s] * scale
        for copy in pair(s):
            copy.wait()
        _, updated = step_of(mean, moved[s], held[s])
        sent[s] = updated.astype(sent.dtype)
        total[s] = mean
        pltpu.make_async_copy(total.at[s], means.at[s], mean_sems.at[s]).start()
        return carry

    lax.fori_loop(0, entries, work, 0)
    leaves = [
        pltpu.make_async_copy(sent.at[pl.ds(k * slots, slots)], fetched[k], sent_sems.at[k]) for k in range(n)
    ]
    for copy in leaves:
        copy.start()

    def end(s, carry):
        pltpu.make_async_copy(total.at[s], means.at[s], mean_sems.at[s]).wait()
        return carry

    lax.fori_loop(0, entries, end, 0)
    for copy in leaves:
        copy.wait()


def listed(start, block_size, facts, params, momentum, received):
    n, (slots, rows, width) = len(received), received[0].shape
    entries = n * slots
    shape = (entries, rows, width)
    out = pl.pallas_call(
        functools.partial(listed_body, start, block_size, params.shape[0] // block_size, n),
        name="listed",
        in_specs=[SMEM, HBM, HBM] + [ANY] * n,
        out_specs=[ANY] * (n + 1),
        out_shape=[jax.ShapeDtypeStruct(piece.shape, piece.dtype) for piece in received]
        + [jax.ShapeDtypeStruct(shape, jnp.float32)],
        scratch_shapes=[
            pltpu.SMEM((entries,), jnp.int32),
            pltpu.SMEM((entries,), jnp.int32),
            pltpu.VMEM(shape, received[0].dtype),
            pltpu.VMEM(shape, params.dtype),
            pltpu.VMEM(shape, momentum.dtype),
            pltpu.VMEM(shape, jnp.float32),
            pltpu.VMEM(shape, received[0].dtype),
            DMA((n,)), DMA((entries,)), DMA((entries,)), DMA((entries,)), DMA((n,)),
        ],
        cost_estimate=pl.CostEstimate(
            flops=10 * entries * rows * width, bytes_accessed=16 * entries * rows * width, transcendentals=0
        ),
    )(facts, params, momentum, *received)
    return out[:n], out[n]


def update_body(block_size, block_count, group, n, parts, facts, params, momentum, *refs):
    means, (params_new, momentum_new) = refs[:parts], refs[parts:]
    entries, rows, _ = means[0].shape
    slots = entries // n
    first = lax.axis_index("expert") * block_count + pl.program_id(0) * group
    moment, updated = step_of(0.0, momentum[...], params[...])
    params_new[...] = updated
    momentum_new[...] = moment.astype(momentum_new.dtype)
    for k in range(n):
        replica = peer_in_kernel(k, n)
        for j in range(slots):
            where = facts[replica, j] - first

            @pl.when(jnp.logical_and(where >= 0, where < group))
            def _(where=where, s=k * slots + j):
                for part in range(parts):
                    span = pl.ds(pl.multiple_of(where * block_size + part * rows, 16), rows)
                    moment, updated = step_of(means[part][s], momentum[span, :], params[span, :])
                    params_new[span, :] = updated
                    momentum_new[span, :] = moment.astype(momentum_new.dtype)


def update(block_size, facts, params, momentum, means):
    rows, width = params.shape
    count = rows // block_size
    group = max(
        k for k in range(1, count + 1)
        if count % k == 0 and (k == 1 or k * block_size * width * 4 <= BLOCK_BYTES)
    )
    spec = pl.BlockSpec((group * block_size, width), lambda i: (i, 0))
    return pl.pallas_call(
        functools.partial(update_body, block_size, count, group, facts.shape[0], len(means)),
        name="update",
        grid=(count // group,),
        in_specs=[SMEM, spec, spec] + [VMEM] * len(means),
        out_specs=[spec, spec],
        out_shape=[
            jax.ShapeDtypeStruct(params.shape, params.dtype),
            jax.ShapeDtypeStruct(momentum.shape, momentum.dtype),
        ],
        cost_estimate=pl.CostEstimate(
            flops=6 * rows * width, bytes_accessed=12 * rows * width, transcendentals=0
        ),
    )(facts, params, momentum, *means)


def blend_body(start, n, count, rows_in, *rest):
    returned, blended = rest[:n], rest[-6]
    got, own, mixed, load_sems, got_sems = rest[-5:-2] + (rest[-2], rest[-1])
    _, slots, rows, width = got.shape
    span = pl.ds(start, rows)
    loads = [
        pltpu.make_async_copy(rows_in.at[:, span, columns_of(k, n, width)], own.at[k], load_sems.at[k])
        for k in range(n)
    ]
    arrivals = [pltpu.make_async_copy(returned[k], got.at[k], got_sems.at[k]) for k in range(n)]
    stores = [
        pltpu.make_async_copy(mixed.at[k], blended.at[:, span, columns_of(k, n, width)], load_sems.at[k])
        for k in range(n)
    ]
    for k in range(n):
        loads[k].start()
        arrivals[k].start()
    for k in range(n):
        loads[k].wait()
        arrivals[k].wait()
        for j in range(slots):
            rows_float = own[k, j].astype(jnp.float32)
            both = blend_weight * rows_float + (1.0 - blend_weight) * got[k, j].astype(jnp.float32)
            mixed[k, j] = jnp.where(count[0] > j, both, rows_float).astype(mixed.dtype)
        stores[k].start()
    for copy in stores:
        copy.wait()


def blend(start, count, returned, rows_in, blended):
    n, (slots, rows, width) = len(returned), returned[0].shape
    before = [] if blended is None else [blended]
    scratch = pltpu.VMEM((n, slots, rows, width), rows_in.dtype)
    return pl.pallas_call(
        functools.partial(blend_body, start, n),
        name="blend",
        in_specs=[SMEM, HBM] + [ANY] * n + [HBM] * len(before),
        out_specs=HBM,
        out_shape=jax.ShapeDtypeStruct(rows_in.shape, rows_in.dtype),
        input_output_aliases={2 + n: 0} if before else {},
        scratch_shapes=[scratch, scratch, scratch, DMA((n,)), DMA((n,))],
    )(count, rows_in, *returned, *before)


def local(outer_params, momentum, replica_deltas, replica_rows, block_ids, slot_counts):
    n = lax.axis_size("replica")
    slots = block_ids.shape[1]
    block_size = replica_deltas.shape[2]
    rows = block_size // PARTS
    deltas, own_rows = replica_deltas[0], replica_rows[0]

    def exchange(pieces):
        out = list(pieces)
        for k in rounds_of(n):
            if k:
                out[k] = lax.ppermute(pieces[k], "replica", [(i, peer_of(i, k, n)) for i in range(n)])
        return out

    received = []
    for part in range(PARTS):
        packed = pack(deltas, part * rows, rows, n)
        received.append(exchange(packed))
    facts = jnp.concatenate([block_ids, slot_counts], axis=1)
    facts = lax.all_to_all(jnp.broadcast_to(facts, (n, slots + 1)), "replica", 0, 0, tiled=True)
    returned, means = [], []
    for part in range(PARTS):
        fetched, mean = listed(part * rows, block_size, facts, outer_params, momentum, received[part])
        means.append(mean)
        returned.append(exchange(fetched))
    params_new, momentum_new = update(block_size, facts, outer_params, momentum, means)
    blended = None
    for part in range(PARTS):
        blended = blend(part * rows, slot_counts[0], returned[part], own_rows, blended)
    return params_new, momentum_new, blended[None]


def solution(mesh):
    in_specs = (
        P("expert", "replica"),
        P("expert", "replica"),
        P("replica", "expert", None, None),
        P("replica", "expert", None, None),
        P("replica", "expert"),
        P("replica", "expert"),
    )
    out_specs = (P("expert", "replica"), P("expert", "replica"), P("replica", "expert", None, None))
    return jax.shard_map(local, mesh=mesh, in_specs=in_specs, out_specs=out_specs, check_vma=False)
```
